512 devices in a mesh: groups: 2 (over y), tp: 16 (over x, core), kv: 16 (over z).
Axes of the slice: x: 8, y: 2, z: 16, core: 2. Of those that a mesh axis runs over, the one named last changes fastest.
The devices are a block of a 8x8x16 slice.
Arguments:
- prompt_rows: bfloat16 [1024, 8192], P('groups', 'kv'), parts along dimension 0, may hold values from -400 to 400
- step_rows: bfloat16 [4, 8192], P('groups', 'kv'), parts along dimension 0, may hold values from -400 to 400
- norm_gain: bfloat16 [8192], P('kv'), may hold values from 0.5 to 1.5
- w_query: bfloat16 [8192, 8192], P('kv', 'tp'), may hold values from -0.0625 to 0.0625
- w_key: bfloat16 [8192, 1024], P('kv', 'tp'), may hold values from -0.125 to 0.125
- w_value: bfloat16 [8192, 1024], P('kv', 'tp'), may hold values from -0.0625 to 0.0625
- w_output: bfloat16 [8192, 8192], P('tp', 'kv'), may hold values from -0.0625 to 0.0625
- kv_cache: bfloat16 [8, 16384, 4096], P('groups', 'kv', 'tp'), parts along dimension 0, may hold values from -250 to 250, as said below
- step_lengths: int32 [4], P('groups'), parts along dimension 0, may hold values from 4096 to 16383
- rollout_ids: int32 [4], P('groups'), parts along dimension 0, may hold values from 0 to 1, each once
- resume_offsets: int32 [4], P('groups'), parts along dimension 0, may hold values from 2048 to 15872
- stretch_rollout: int32 [1024], P('groups'), parts along dimension 0, may hold values from 0 to 1, never falling along the last dimension, each value on 1 to 384 neighbouring positions
Outputs:
- prompt_out: bfloat16 [1024, 8192], P(('groups', 'tp'), 'kv'), parts along dimension 0
- step_out: bfloat16 [4, 8192], P('groups', 'kv'), parts along dimension 0
The draws below stay inside these ranges and needn't reach their ends.
There are 2 independent parts, one for each index of `groups`. The reference program is written for one: setup_inputs(seed, part) draws one part's arguments, and reference() takes and returns one part's arrays. A program takes and returns all parts, laid end to end along the dimension named above; an argument that names none is the same for every part. Nothing has to cross between parts.
Inputs may be any that keep to these rules, and one draw needn't show every extreme that they name: `kv_cache`: along the last dimension, block t of 16 holds for each j below 1 the keys then the values (128 entries each) of key-value head (t * 4) // 8 + j; blocks naming the same head are equal.
All inputs are finite; a program needn't handle non-finite values.
Results may differ from the reference program's by a relative error of at most 0.012.
The reference program's roundings to bfloat16 on the way count: a program that leaves them out, or rounds other values in their place, can miss the bound.
Values may be sent and summed in bfloat16 or wider, within the bound.
A program may use at most 64 MiB of HBM per device.

```python
import math
import jax
import jax.numpy as jnp
import numpy as np
from jax import lax

D = 8192
H = 64
KVH = 8
HD = 128
STRETCH = 512
SEQS = 2
ROLL = 2
LMAX = 16384
QPK = 8
HQL = 4
KV_DEV = 1
SLOTS = 4
SEG_MOST = 384
N_TP = 16


def activation(key, row_count):
    key_base = jax.random.fold_in(key, 0)
    column = jnp.exp(jnp.arange(D, dtype=jnp.float32) * (math.log(3.0) / D))
    base_draw = jnp.clip(jax.random.normal(key_base, (row_count, D), jnp.float32), -5.0, 5.0)
    result = base_draw * column[None, :]
    return result.astype(jnp.bfloat16)


def draw_prompt_rows(key, part):
    return activation(jax.random.fold_in(key, 11), STRETCH)


def draw_step_rows(key, part):
    return activation(jax.random.fold_in(key, 13), SEQS)


def draw_kv_cache(key, part):
    key_base = jax.random.fold_in(jax.random.fold_in(key, 17), 0)
    full_shape = (SLOTS, LMAX, KVH, 2, HD)
    kind_scale = jnp.array([2.0, 1.0], jnp.float32)[None, None, None, :, None]
    canon = jnp.clip(jax.random.normal(key_base, full_shape, jnp.float32), -4.0, 4.0) * kind_scale
    head_table = np.array([tp_rank * HQL // QPK + local for tp_rank in range(N_TP) for local in range(KV_DEV)], dtype=np.int32)
    copied = canon[:, :, head_table]
    return copied.reshape(SLOTS, LMAX, N_TP * KV_DEV * 2 * HD).astype(jnp.bfloat16)


def levels(own_key, dims, shards, least, high):
    gain, own = 1.0, jax.random.fold_in(own_key, 6)
    for dim, parts in shards:
        heights = jnp.exp(jax.random.uniform(jax.random.fold_in(own, dim), (parts,), jnp.float32, least / len(shards), high / len(shards)))
        gain = gain * jnp.repeat(heights, dims[dim] // parts).reshape([-1 if axis == dim else 1 for axis in range(len(dims))])
    return gain


def split_up(count, total, limit, skew):
    weights = [(1 << 20) // math.isqrt(standing ** skew) + 1 for standing in range(2, count + 1)]
    rest, given = total - limit - (count - 1), [1] * (count - 1)
    while rest > 0:
        movable = [i for i in range(count - 1) if given[i] < limit]
        whole, budget = sum([weights[i] for i in movable]), rest
        for i in movable:
            extra = min(limit - given[i], max(1, budget * weights[i] // whole), rest)
            given[i] = given[i] + extra
            rest = rest - extra
    return np.array([limit] + given)


def uneven(key, count, total, limit, slope):
    if count == 2:
        one = jax.random.randint(key, (), max(1, total - limit), min(limit, total - 1) + 1)
        return jnp.stack([one, total - one])
    tallies = jnp.asarray(split_up(count, total, limit, slope), jnp.int32)
    pairs = (count - 1) // 2
    source_of, taker = tallies[1:1 + 2 * pairs:2], tallies[2:2 + 2 * pairs:2]
    room = jnp.minimum(source_of - 1, limit - taker)
    moved = jax.random.randint(jax.random.fold_in(key, 1), (pairs,), 0, 1 << 20) % (room + 1)
    tallies = tallies.at[1:1 + 2 * pairs:2].set(source_of - moved).at[2:2 + 2 * pairs:2].set(taker + moved)
    return tallies[jax.random.permutation(jax.random.fold_in(key, 2), count)]


def bell_draw(rng, extent, width, bound, shards=(), kind=jnp.bfloat16):
    drawn = width * jax.random.normal(rng, extent, jnp.float32)
    if shards:
        drawn = drawn * levels(rng, extent, shards, -0.22, 0.18)
    return jnp.clip(drawn, -bound, bound).astype(kind)


def setup_inputs(seed: int = 0, part: int = 0) -> dict:
    splits = jax.random.split(jax.random.key(seed), 13)
    part_splits = jax.random.split(jax.random.fold_in(splits[12], part), 13)
    return {
        "prompt_rows": draw_prompt_rows(jax.random.fold_in(jax.random.fold_in(splits[12], part), 71), part),
        "step_rows": draw_step_rows(jax.random.fold_in(jax.random.fold_in(splits[12], part), 71), part),
        "norm_gain": jnp.clip(1.0 + 0.1 * jax.random.normal(splits[2], (D,), jnp.float32), 0.5, 1.5).astype(jnp.bfloat16),
        "w_query": bell_draw(splits[3], (D, H * HD), D ** -0.5, 0.0625, ((0, 16), (1, 16))),
        "w_key": bell_draw(splits[4], (D, KVH * HD), (D // 4) ** -0.5, 0.125, ((0, 16), (1, 16))),
        "w_value": bell_draw(splits[5], (D, KVH * HD), D ** -0.5, 0.0625, ((0, 16), (1, 16))),
        "w_output": bell_draw(splits[6], (H * HD, D), (H * HD) ** -0.5, 0.0625, ((0, 16), (1, 16))),
        "kv_cache": draw_kv_cache(jax.random.fold_in(jax.random.fold_in(splits[12], part), 71), part),
        "step_lengths": jax.random.randint(part_splits[8], (SEQS,), LMAX // 4, LMAX).astype(jnp.int32),
        "rollout_ids": jax.random.permutation(part_splits[9], ROLL).astype(jnp.int32),
        "resume_offsets": jax.random.randint(part_splits[10], (ROLL,), LMAX // 8, LMAX - STRETCH + 1).astype(jnp.int32),
        "stretch_rollout": jnp.searchsorted(jnp.cumsum(uneven(part_splits[11], ROLL, STRETCH, SEG_MOST, 0)), jnp.arange(STRETCH), side="right").astype(jnp.int32),
    }


EPSILON = 1e-05
THETA = 500000.0
NEGATIVE = -1e+30

def rotate(values, positions):
    half_dim = values.shape[-1] // 2
    freq_index = jnp.arange(half_dim, dtype=jnp.float32)
    inverse = jnp.exp(freq_index * (-2.0 * math.log(THETA) / values.shape[-1]))
    angles = positions.astype(jnp.float32)[:, None] * inverse[None, :]
    cosine = jnp.cos(angles)[:, None, :]
    sine_part = jnp.sin(angles)[:, None, :]
    first_half = values[..., :half_dim]
    second_half = values[..., half_dim:]
    return jnp.concatenate([first_half * cosine - second_half * sine_part, second_half * cosine + first_half * sine_part], axis=-1)

def stretch_positions(stretch_rollout, resume_offsets):
    members = jnp.arange(resume_offsets.shape[0], dtype=jnp.int32)
    onehot = (stretch_rollout[:, None] == members[None, :]).astype(jnp.int32)
    starts = lax.optimization_barrier(jnp.sum((stretch_rollout[:, None] < members[None, :]).astype(jnp.int32), axis=0))
    shifted = lax.optimization_barrier(jnp.sum(onehot * (resume_offsets - starts)[None, :], axis=1))
    return shifted + jnp.arange(stretch_rollout.shape[0], dtype=jnp.int32)

def normalized_mix(scores, allowed, values, form):
    masked = jnp.where(allowed, scores, NEGATIVE)
    top_score = lax.optimization_barrier(jnp.max(masked, axis=-1, keepdims=True))
    weights = jnp.where(allowed, jnp.exp(scores - top_score), 0.0)
    denominator = lax.optimization_barrier(jnp.sum(weights, axis=-1))
    rounded = lax.optimization_barrier(weights.astype(jnp.bfloat16)).astype(jnp.float32)
    mixed_out = jnp.einsum(form, rounded, values.astype(jnp.float32))
    return (mixed_out / denominator[..., None]).astype(jnp.bfloat16)

def reference(prompt_rows, step_rows, norm_gain, w_query, w_key, w_value, w_output, kv_cache, step_lengths, rollout_ids, resume_offsets, stretch_rollout):
    all_rows = jnp.concatenate([prompt_rows, step_rows], axis=0)
    widened = all_rows.astype(jnp.float32)
    norm_scale = lax.rsqrt(lax.optimization_barrier(jnp.sum(widened * widened, axis=1)) / D + EPSILON)
    normed = (widened * norm_gain.astype(jnp.float32)[None, :]).astype(jnp.bfloat16)
    row_count = all_rows.shape[0]
    query_raw = jnp.dot(normed, w_query, preferred_element_type=jnp.float32) * norm_scale[:, None]
    key_raw = jnp.dot(normed, w_key, preferred_element_type=jnp.float32) * norm_scale[:, None]
    value_rows = (jnp.dot(normed, w_value, preferred_element_type=jnp.float32) * norm_scale[:, None]).astype(jnp.bfloat16)
    value_rows = lax.optimization_barrier(value_rows).reshape(row_count, KVH, HD)
    positions = jnp.concatenate([stretch_positions(stretch_rollout, resume_offsets), step_lengths.astype(jnp.int32)])
    query_rows = lax.optimization_barrier(rotate(query_raw.reshape(row_count, H, HD), positions).astype(jnp.bfloat16))
    key_rows = lax.optimization_barrier(rotate(key_raw.reshape(row_count, KVH, HD), positions).astype(jnp.bfloat16))
    layout = kv_cache.reshape(SLOTS, LMAX, N_TP, KV_DEV, 2, HD)
    owners = np.array([kv_head * QPK // HQL for kv_head in range(KVH)], dtype=np.int32)
    within = np.array([kv_head - kv_head * QPK // HQL * HQL // QPK for kv_head in range(KVH)], dtype=np.int32)
    canon = layout[:, :, owners, within]
    rollout_cache = canon[SEQS + rollout_ids.astype(jnp.int32)]
    step_cache = canon[:SEQS]
    members = jnp.arange(ROLL, dtype=jnp.int32)
    key_index = jnp.arange(LMAX, dtype=jnp.int32)
    in_member = stretch_rollout[:, None] == members[None, :]
    before = key_index[None, :] < resume_offsets[:, None]
    cache_mask = (in_member[:, :, None] & before[None, :, :]).reshape(STRETCH, ROLL * LMAX)
    stretch_index = jnp.arange(STRETCH, dtype=jnp.int32)
    stretch_mask = (stretch_rollout[:, None] == stretch_rollout[None, :]) & (stretch_index[None, :] <= stretch_index[:, None])
    prompt_mask = jnp.concatenate([cache_mask, stretch_mask], axis=1)[:, None, :]
    step_mask = jnp.concatenate([key_index[None, :] < step_lengths[:, None], jnp.ones((SEQS, 1), dtype=bool)], axis=1)[:, None, :]
    inverse_root = 1.0 / math.sqrt(HD)

    def one_head(kv_head):
        group_query = lax.dynamic_slice_in_dim(query_rows, kv_head * QPK, QPK, 1).astype(jnp.float32)
        own_keys = lax.dynamic_index_in_dim(key_rows, kv_head, 1, keepdims=False)
        own_values = lax.dynamic_index_in_dim(value_rows, kv_head, 1, keepdims=False)
        head_cache = lax.dynamic_index_in_dim(rollout_cache, kv_head, 2, keepdims=False)
        prompt_keys = jnp.concatenate([head_cache[:, :, 0].reshape(ROLL * LMAX, HD), own_keys[:STRETCH]], axis=0)
        prompt_values = jnp.concatenate([head_cache[:, :, 1].reshape(ROLL * LMAX, HD), own_values[:STRETCH]], axis=0)
        prompt_scores = jnp.einsum('qgd,kd->qgk', group_query[:STRETCH], prompt_keys.astype(jnp.float32)) * inverse_root
        prompt_mix = normalized_mix(prompt_scores, prompt_mask, prompt_values, 'qgk,kd->qgd')
        step_head = lax.dynamic_index_in_dim(step_cache, kv_head, 2, keepdims=False)
        step_keys = jnp.concatenate([step_head[:, :, 0], own_keys[STRETCH:][:, None, :]], axis=1)
        step_values = jnp.concatenate([step_head[:, :, 1], own_values[STRETCH:][:, None, :]], axis=1)
        step_scores = jnp.einsum('sgd,skd->sgk', group_query[STRETCH:], step_keys.astype(jnp.float32)) * inverse_root
        step_mix = normalized_mix(step_scores, step_mask, step_values, 'sgk,skd->sgd')
        return (prompt_mix, step_mix)
    prompt_mix, step_mix = lax.map(one_head, jnp.arange(KVH, dtype=jnp.int32))
    prompt_mix = jnp.transpose(prompt_mix, (1, 0, 2, 3)).reshape(STRETCH, H * HD)
    step_mix = jnp.transpose(step_mix, (1, 0, 2, 3)).reshape(SEQS, H * HD)
    prompt_out = jnp.dot(prompt_mix, w_output, preferred_element_type=jnp.float32).astype(jnp.bfloat16)
    step_out = jnp.dot(step_mix, w_output, preferred_element_type=jnp.float32).astype(jnp.bfloat16)
    return (prompt_out, step_out)
```

```python
import functools
import math

import jax
import jax.numpy as jnp
import numpy as np
from jax import lax
from jax.experimental import pallas as pl
from jax.experimental.pallas import tpu as pltpu
from jax.sharding import PartitionSpec as P

HD = 128
SEQS = 2
EPSILON = 1e-05
THETA = 500000.0
NEGATIVE = -1e30
EXPONENT = math.log2(math.e) / math.sqrt(HD)
F32, BF16 = jnp.float32, jnp.bfloat16
MESH = pl.DeviceIdType.MESH


def iota(shape, dim):
    return lax.broadcasted_iota(jnp.int32, shape, dim)


def dot(a, b):
    return jnp.dot(a, b, preferred_element_type=F32)


def dot_t(a, b):
    return lax.dot_general(a, b, (((1,), (1,)), ((), ())), preferred_element_type=F32)


def far_first(me, count, j):
    distance = count // 2 - (j + 1) // 2
    return lax.rem(me + distance * (2 * lax.rem(j, 2) - 1) + count, count)


def high_low(value):
    high = value.astype(BF16).astype(F32)
    return high, value - high


def rotated(value, cosine, sine):
    return value * cosine + pltpu.roll(value, HD // 2, 1) * sine


def angles(position, inverse):
    angle = position * inverse
    lane = iota(angle.shape, 1)
    sine = jnp.sin(angle)
    return jnp.cos(angle), jnp.where(lane < HD // 2, -sine, sine)


def stacked(rows):
    return jnp.concatenate([rows[:, at : at + HD] for at in range(0, rows.shape[1], HD)], axis=0)


def attend(queries, second, allowed, keys, values):
    both = jnp.concatenate(
        [jnp.where(second, 0.0, queries), jnp.where(second, queries, 0.0)], axis=1
    ).astype(BF16)
    scores = jnp.where(allowed, dot_t(both, keys), NEGATIVE)
    top = jnp.max(scores, axis=1, keepdims=True)
    weights = jnp.exp2((scores - top) * EXPONENT)
    total = jnp.sum(weights, axis=1, keepdims=True)
    mixed = dot(weights.astype(BF16), values)
    mixed = jnp.where(second, mixed[:, HD:], mixed[:, :HD])
    some = top > 0.1 * NEGATIVE
    return jnp.where(some, mixed, 0.0), top, jnp.where(some, total, 0.0)


def packed(mixed, top, total, rows):
    heads = mixed.shape[0] // rows
    lane = iota((rows, HD), 1)
    tile = jnp.zeros((rows, HD), F32)
    high, rest = high_low(top)
    middle, low = high_low(rest)
    total_high, total_low = high_low(total)
    for k, column in enumerate((high, middle, low, total_high, total_low)):
        for h in range(heads):
            tile = jnp.where(lane == k * heads + h, column[h * rows : (h + 1) * rows], tile)
    return jnp.concatenate(
        [mixed[h * rows : (h + 1) * rows] for h in range(heads)] + [tile], axis=1
    ).astype(BF16)


def combined(parts_ref, count):
    width = parts_ref.shape[2] - HD
    heads = width // HD
    tops, totals = [], []
    for s in range(count):
        tile = parts_ref[s, :, width:].astype(F32)
        shift = lambda k: pltpu.roll(tile, HD - k * heads, 1)
        tops.append(tile + shift(1) + shift(2))
        totals.append(shift(3) + shift(4))
    top = functools.reduce(jnp.maximum, tops)
    weights = [jnp.exp2((t - top) * EXPONENT) for t in tops]
    total = functools.reduce(jnp.add, [w * t for w, t in zip(weights, totals)])
    outs = []
    for h in range(heads):
        mixed = 0.0
        for s in range(count):
            mixed += weights[s][:, h : h + 1] * parts_ref[s, :, h * HD : (h + 1) * HD].astype(F32)
        outs.append(mixed / total[:, h : h + 1])
    return jnp.concatenate(outs, axis=1)


def kernel(
    kv_count,
    tp_count,
    rows_ref,
    step_ref,
    gain_ref,
    wq_ref,
    wk_ref,
    wv_ref,
    wo_hbm,
    cache_hbm,
    lengths_ref,
    ids_ref,
    offsets_ref,
    rollout_ref,
    inverse_ref,
    out_ref,
    step_out_ref,
    wo_ref,
    cache_ref,
    a_send,
    a_recv,
    aux_recv,
    pair_send,
    pair_recv,
    q_recv,
    c_send,
    c_recv,
    cs_recv,
    m_recv,
    e_send,
    e_recv,
    es_recv,
    keys_ref,
    values_ref,
    step_keys_ref,
    step_values_ref,
    local_sem,
    pair_sem,
    send_sem,
    recv_sem,
):
    me = lax.axis_index("kv")
    tp = lax.axis_index("tp")
    features = rows_ref.shape[1]
    row_count = rows_ref.shape[0]
    width = wq_ref.shape[1]
    heads = width // HD
    share = row_count // kv_count
    block = cache_ref.shape[1]
    total_features = features * kv_count
    partner = tp + 1 - 2 * lax.rem(tp, 2)

    wo_copy = pltpu.make_async_copy(wo_hbm, wo_ref, local_sem.at[0])
    cache_copy = pltpu.make_async_copy(cache_hbm, cache_ref, local_sem.at[1])
    wo_copy.start()
    cache_copy.start()

    barrier = pltpu.get_barrier_semaphore()

    def greet(axis, count, here):
        def one(j, carry):
            pl.semaphore_signal(
                barrier,
                inc=1,
                device_id={axis: far_first(here, count, j)},
                device_id_type=MESH,
            )
            return carry

        lax.fori_loop(0, count - 1, one, 0)

    greet("kv", kv_count, me)
    greet("tp", tp_count, tp)

    def remote(phase, axis, peer, source, slot_ref, slot):
        return pltpu.make_async_remote_copy(
            src_ref=source,
            dst_ref=slot_ref.at[slot],
            send_sem=send_sem.at[phase, peer],
            recv_sem=recv_sem.at[phase, slot],
            device_id={axis: peer},
            device_id_type=MESH,
        )

    def to_all(phase, axis, count, here, source, slot_ref):
        def one(j, carry):
            peer = far_first(here, count, j)
            remote(phase, axis, peer, source(peer), slot_ref, here).start()
            return carry

        lax.fori_loop(0, count - 1, one, 0)

    def arrive(phase, axis, peer, slot_ref):
        remote(phase, axis, peer, slot_ref.at[peer], slot_ref, peer).wait_recv()

    def all_arrive(phase, axis, count, here, slot_ref):
        def one(j, carry):
            arrive(phase, axis, far_first(here, count, j), slot_ref)
            return carry

        lax.fori_loop(0, count - 1, one, 0)

    def all_sent(phase, axis, count, here, source, slot_ref):
        def one(j, carry):
            peer = far_first(here, count, j)
            remote(phase, axis, peer, source(peer), slot_ref, here).wait_send()
            return carry

        lax.fori_loop(0, count - 1, one, 0)

    gain = gain_ref[...].astype(F32)
    wide = rows_ref[...].astype(F32)
    normed = (wide * gain).astype(BF16)
    step_wide = jnp.concatenate(
        [step_ref[...].astype(F32), jnp.zeros((HD - SEQS, features), F32)], axis=0
    )
    step_normed = (step_wide[:16] * gain).astype(BF16)
    ones = jnp.ones((8, features), BF16)

    def squares(value):
        high, low = high_low(value * value)
        return dot_t(ones, high.astype(BF16)) + dot_t(ones, low.astype(BF16))

    weight_pair = jnp.concatenate([wk_ref[...], wv_ref[...]], axis=1)
    square_high, square_low = high_low(
        jnp.concatenate([squares(wide), squares(step_wide)], axis=1)
    )
    step_part = jnp.concatenate(
        [dot(step_normed, wq_ref[...])[:8], dot(step_normed, weight_pair)[:8]], axis=1
    )
    aux_row = iota(step_part.shape, 0)
    aux = jnp.where(
        aux_row == SEQS, square_high, jnp.where(aux_row == SEQS + 1, square_low, step_part)
    )
    aux_recv[me] = aux.astype(BF16)
    a_send[:, :, :width] = dot(normed, wq_ref[...]).astype(BF16).reshape(kv_count, share, width)
    a_send[:, :, width:] = dot(normed, weight_pair).astype(BF16).reshape(kv_count, share, HD)
    a_recv[me] = a_send[me]

    pl.semaphore_wait(barrier, kv_count + tp_count - 2)
    aux_source = lambda peer: aux_recv.at[me]
    a_source = lambda peer: a_send.at[peer]
    to_all(0, "kv", kv_count, me, aux_source, aux_recv)
    to_all(1, "kv", kv_count, me, a_source, a_recv)

    cache_copy.wait()
    keys_ref[:block, :HD] = cache_ref[SEQS + ids_ref[0], :, :HD]
    keys_ref[:block, HD:] = cache_ref[SEQS + ids_ref[1], :, :HD]
    values_ref[:block, :HD] = cache_ref[SEQS + ids_ref[0], :, HD:]
    values_ref[:block, HD:] = cache_ref[SEQS + ids_ref[1], :, HD:]
    step_keys_ref[:block, :HD] = cache_ref[0, :, :HD]
    step_keys_ref[:block, HD:] = cache_ref[1, :, :HD]
    step_values_ref[:block, :HD] = cache_ref[0, :, HD:]
    step_values_ref[:block, HD:] = cache_ref[1, :, HD:]
    wo_copy.wait()

    first_count = jnp.sum(
        jnp.sum((rollout_ref[...] == 0).astype(F32), axis=1, keepdims=True), axis=0, keepdims=True
    )
    offset_0 = offsets_ref[0].astype(F32)
    offset_1 = offsets_ref[1].astype(F32)
    own_row = (iota((share, 1), 0) + me * share).astype(F32)
    position = jnp.where(own_row >= first_count, own_row + offset_1 - first_count, own_row + offset_0)
    step_row = iota((8, 1), 0)
    step_position = jnp.where(step_row == 0, lengths_ref[0], lengths_ref[1]).astype(F32)
    inverse = inverse_ref[...]
    cosine, sine = angles(position, inverse)
    step_cosine, step_sine = angles(step_position, inverse)

    all_arrive(0, "kv", kv_count, me, aux_recv)
    aux_sum = aux_recv[0].astype(F32)
    for s in range(1, kv_count):
        aux_sum += aux_recv[s].astype(F32)
    square_row = aux_sum[SEQS : SEQS + 1] + aux_sum[SEQS + 1 : SEQS + 2]

    def own_scale(start, rows):
        shape = (rows, square_row.shape[1])
        mine = iota(shape, 1) == start + iota(shape, 0)
        squared = jnp.sum(jnp.where(mine, square_row, 0.0), axis=1, keepdims=True)
        return lax.rsqrt(squared / total_features + EPSILON)

    scale = own_scale(me * share, share)
    step_scale = own_scale(row_count, 8)
    step_raw = aux_sum * step_scale

    all_arrive(1, "kv", kv_count, me, a_recv)
    raw = a_recv[0].astype(F32)
    for s in range(1, kv_count):
        raw += a_recv[s].astype(F32)
    raw = raw * scale

    pair = jnp.concatenate([raw[:, width:], step_raw[:, width:]], axis=0)
    pair_send[...] = pair
    pair_copy = pltpu.make_async_remote_copy(
        src_ref=pair_send,
        dst_ref=pair_recv,
        send_sem=pair_sem.at[0],
        recv_sem=pair_sem.at[1],
        device_id={"tp": partner},
        device_id_type=MESH,
    )
    pair_copy.start()
    q_recv[me] = jnp.concatenate(
        [rotated(raw[:, at : at + HD], cosine, sine) for at in range(0, width, HD)], axis=1
    ).astype(BF16)
    q_source = lambda peer: q_recv.at[me]
    to_all(2, "kv", kv_count, me, q_source, q_recv)

    step_queries = jnp.concatenate(
        [rotated(step_raw[:, at : at + HD], step_cosine, step_sine) for at in range(0, width, HD)],
        axis=0,
    )

    pair_copy.wait()
    other = pair_recv[...]
    lane = iota(other.shape, 1)
    even = iota(other.shape, 0) * 0 + lax.rem(tp, 2) == 0
    left = jnp.where(even, pair, other)
    right = jnp.where(even, other, pair)
    key_raw = jnp.where(lane < HD // 2, left, pltpu.roll(right, HD // 2, 1))
    value_rows = jnp.where(lane < HD // 2, pltpu.roll(left, HD // 2, 1), right)
    own_keys = rotated(key_raw[:share], cosine, sine)
    step_keys = rotated(key_raw[share:], step_cosine, step_sine)

    def tail(rows):
        filled = jnp.concatenate([rows, jnp.zeros((HD - rows.shape[0], HD), F32)], axis=0)
        return jnp.concatenate([filled, filled], axis=1).astype(BF16)

    keys_ref[block:, :] = tail(own_keys)
    values_ref[block:, :] = tail(value_rows[:share])
    step_keys_ref[block:, :] = tail(step_keys)
    step_values_ref[block:, :] = tail(value_rows[share:])

    key_count = block + HD
    key_lane = iota((1, key_count), 1)
    key_position = key_lane + me * block
    stack_row = iota((heads * 8, 1), 0)
    sequence = lax.rem(stack_row, 8)
    step_limit = jnp.where(sequence == 0, lengths_ref[0], lengths_ref[1])
    own_lane = jnp.where(key_lane * 0 + me == 0, key_lane - block, -1)
    step_allowed = ((key_lane < block) & (key_position < step_limit)) | (own_lane == sequence)
    step_mixed = attend(
        step_queries, sequence > 0, step_allowed, step_keys_ref[...], step_values_ref[...]
    )
    cs_recv[me] = packed(*step_mixed, 8)
    cs_source = lambda peer: cs_recv.at[me]
    to_all(3, "kv", kv_count, me, cs_source, cs_recv)

    row_in_chunk = lax.rem(iota((heads * share, 1), 0), share)

    def one_chunk(j, carry):
        owner = jnp.where(j == 0, me, far_first(me, kv_count, j - 1))

        @pl.when(j > 0)
        def _():
            arrive(2, "kv", owner, q_recv)

        row = row_in_chunk + owner * share
        second = row.astype(F32) >= first_count
        limit = jnp.where(second, offsets_ref[1], offsets_ref[0])
        tail_key = key_lane[:, block:] - block + me * share
        tail_second = tail_key.astype(F32) >= first_count
        allowed = jnp.concatenate(
            [
                (key_position[:, :block] < limit).astype(F32),
                jnp.where(
                    (tail_key <= row)
                    & (tail_key < (me + 1) * share)
                    & (tail_second.astype(F32) == second.astype(F32)),
                    1.0,
                    0.0,
                ),
            ],
            axis=1,
        )
        queries = stacked(q_recv[owner].astype(F32))
        mixed = attend(queries, second, allowed > 0.5, keys_ref[...], values_ref[...])
        message = packed(*mixed, share)

        @pl.when(j == 0)
        def _():
            c_recv[me] = message

        @pl.when(j > 0)
        def _():
            c_send[owner] = message
            remote(4, "kv", owner, c_send.at[owner], c_recv, me).start()

        return carry

    lax.fori_loop(0, kv_count, one_chunk, 0)

    all_arrive(3, "kv", kv_count, me, cs_recv)
    step_mix = combined(cs_recv, kv_count)
    step_mix = jnp.concatenate([step_mix, jnp.zeros_like(step_mix)], axis=0).astype(BF16)
    es_recv[tp] = dot(step_mix, wo_ref[...])[:8].astype(BF16)
    es_source = lambda peer: es_recv.at[tp]
    to_all(5, "tp", tp_count, tp, es_source, es_recv)

    all_arrive(4, "kv", kv_count, me, c_recv)
    m_recv[me] = combined(c_recv, kv_count).astype(BF16)
    m_source = lambda peer: m_recv.at[me]
    to_all(6, "kv", kv_count, me, m_source, m_recv)

    def one_product(j, carry):
        owner = jnp.where(j == 0, me, far_first(me, kv_count, j - 1))

        @pl.when(j > 0)
        def _():
            arrive(6, "kv", owner, m_recv)

        product = dot(m_recv[owner], wo_ref[...]).astype(BF16)

        @pl.when(owner == tp)
        def _():
            e_recv[tp] = product

        @pl.when(owner != tp)
        def _():
            e_send[owner] = product
            remote(7, "tp", owner, e_send.at[owner], e_recv, tp).start()

        return carry

    lax.fori_loop(0, kv_count, one_product, 0)

    all_arrive(5, "tp", tp_count, tp, es_recv)
    step_total = es_recv[0].astype(F32)
    for s in range(1, tp_count):
        step_total += es_recv[s].astype(F32)
    step_out_ref[...] = step_total[:SEQS].astype(BF16)
    all_arrive(7, "tp", tp_count, tp, e_recv)
    total = e_recv[0].astype(F32)
    for s in range(1, tp_count):
        total += e_recv[s].astype(F32)
    out_ref[...] = total.astype(BF16)

    all_sent(0, "kv", kv_count, me, aux_source, aux_recv)
    all_sent(1, "kv", kv_count, me, a_source, a_recv)
    all_sent(2, "kv", kv_count, me, q_source, q_recv)
    all_sent(3, "kv", kv_count, me, cs_source, cs_recv)
    all_sent(4, "kv", kv_count, me, lambda peer: c_send.at[peer], c_recv)
    all_sent(5, "tp", tp_count, tp, es_source, es_recv)
    all_sent(6, "kv", kv_count, me, m_source, m_recv)
    all_sent(7, "tp", tp_count, tp, lambda peer: e_send.at[peer], e_recv)


def on_device(
    prompt_rows,
    step_rows,
    norm_gain,
    w_query,
    w_key,
    w_value,
    w_output,
    kv_cache,
    step_lengths,
    rollout_ids,
    resume_offsets,
    stretch_rollout,
):
    kv_count = lax.axis_size("kv")
    tp_count = lax.axis_size("tp")
    row_count, features = prompt_rows.shape
    width = w_query.shape[1]
    out_width = w_output.shape[1]
    share = row_count // kv_count
    key_count = kv_cache.shape[1] + HD
    frequency = np.exp(np.arange(HD // 2) * (-2.0 * math.log(THETA) / HD)).astype(np.float32)
    inverse = jnp.asarray(np.concatenate([frequency, frequency])[None, :])
    vmem = pl.BlockSpec(memory_space=pltpu.VMEM)
    smem = pl.BlockSpec(memory_space=pltpu.SMEM)
    anywhere = pl.BlockSpec(memory_space=pl.ANY)
    scratch = [
        pltpu.VMEM(w_output.shape, BF16),
        pltpu.VMEM(kv_cache.shape, BF16),
        pltpu.VMEM((kv_count, share, width + HD), BF16),
        pltpu.VMEM((kv_count, share, width + HD), BF16),
        pltpu.VMEM((kv_count, 8, width + HD), BF16),
        pltpu.VMEM((share + 8, HD), F32),
        pltpu.VMEM((share + 8, HD), F32),
        pltpu.VMEM((kv_count, share, width), BF16),
        pltpu.VMEM((kv_count, share, width + HD), BF16),
        pltpu.VMEM((kv_count, share, width + HD), BF16),
        pltpu.VMEM((kv_count, 8, width + HD), BF16),
        pltpu.VMEM((kv_count, share, width), BF16),
        pltpu.VMEM((tp_count, share, out_width), BF16),
        pltpu.VMEM((tp_count, share, out_width), BF16),
        pltpu.VMEM((tp_count, 8, out_width), BF16),
        pltpu.VMEM((key_count, 2 * HD), BF16),
        pltpu.VMEM((key_count, 2 * HD), BF16),
        pltpu.VMEM((key_count, 2 * HD), BF16),
        pltpu.VMEM((key_count, 2 * HD), BF16),
        pltpu.SemaphoreType.DMA((2,)),
        pltpu.SemaphoreType.DMA((2,)),
        pltpu.SemaphoreType.DMA((8, kv_count)),
        pltpu.SemaphoreType.DMA((8, kv_count)),
    ]
    return pl.pallas_call(
        functools.partial(kernel, kv_count, tp_count),
        out_shape=(
            jax.ShapeDtypeStruct((share, out_width), BF16),
            jax.ShapeDtypeStruct((step_rows.shape[0], out_width), BF16),
        ),
        in_specs=[vmem] * 6 + [anywhere] * 2 + [smem] * 3 + [vmem] * 2,
        out_specs=(vmem, vmem),
        scratch_shapes=scratch,
        compiler_params=pltpu.CompilerParams(
            collective_id=0, has_side_effects=True, vmem_limit_bytes=48 * 1024 * 1024
        ),
    )(
        prompt_rows,
        step_rows,
        norm_gain.reshape(1, -1),
        w_query,
        w_key,
        w_value,
        w_output,
        kv_cache,
        step_lengths,
        rollout_ids,
        resume_offsets,
        stretch_rollout.reshape(-1, HD),
        inverse,
    )


def solution(mesh):
    in_specs = (
        P("groups", "kv"),
        P("groups", "kv"),
        P("kv"),
        P("kv", "tp"),
        P("kv", "tp"),
        P("kv", "tp"),
        P("tp", "kv"),
        P("groups", "kv", "tp"),
        P("groups"),
        P("groups"),
        P("groups"),
        P("groups"),
    )
    out_specs = (P(("groups", "tp"), "kv"), P("groups", "kv"))
    return jax.shard_map(
        on_device, mesh=mesh, in_specs=in_specs, out_specs=out_specs, check_vma=False
    )
```

```python
import functools
import math

import jax
import jax.numpy as jnp
import numpy as np
from jax import lax
from jax.experimental import pallas as pl
from jax.experimental.pallas import tpu as pltpu
from jax.sharding import PartitionSpec as P

HD = 128
SEQS = 2
EPSILON = 1e-05
THETA = 500000.0
NEGATIVE = -1e30
EXPONENT = math.log2(math.e) / math.sqrt(HD)
F32, BF16 = jnp.float32, jnp.bfloat16
MESH = pl.DeviceIdType.MESH


def iota(shape, dim):
    return lax.broadcasted_iota(jnp.int32, shape, dim)


def dot(a, b):
    return jnp.dot(a, b, preferred_element_type=F32)


def dot_t(a, b):
    return lax.dot_general(a, b, (((1,), (1,)), ((), ())), preferred_element_type=F32)


def far_first(me, count, j):
    distance = count // 2 - (j + 1) // 2
    return lax.rem(me + distance * (2 * lax.rem(j, 2) - 1) + count, count)


def high_low(value):
    high = value.astype(BF16).astype(F32)
    return high, value - high


def rotated(value, cosine, sine):
    return value * cosine + pltpu.roll(value, HD // 2, 1) * sine


def angles(position, inverse):
    angle = position * inverse
    lane = iota(angle.shape, 1)
    sine = jnp.sin(angle)
    return jnp.cos(angle), jnp.where(lane < HD // 2, -sine, sine)


def stacked(rows):
    return jnp.concatenate([rows[:, at : at + HD] for at in range(0, rows.shape[1], HD)], axis=0)


def attend(queries, second, allowed, keys, values):
    both = jnp.concatenate(
        [jnp.where(second, 0.0, queries), jnp.where(second, queries, 0.0)], axis=1
    ).astype(BF16)
    scores = jnp.where(allowed, dot_t(both, keys), NEGATIVE)
    top = jnp.max(scores, axis=1, keepdims=True)
    weights = jnp.exp2((scores - top) * EXPONENT)
    total = jnp.sum(weights, axis=1, keepdims=True)
    mixed = dot(weights.astype(BF16), values)
    mixed = jnp.where(second, mixed[:, HD:], mixed[:, :HD])
    some = top > 0.1 * NEGATIVE
    return jnp.where(some, mixed, 0.0), top, jnp.where(some, total, 0.0)


def packed(mixed, top, total, rows):
    heads = mixed.shape[0] // rows
    lane = iota((rows, HD), 1)
    tile = jnp.zeros((rows, HD), F32)
    high, rest = high_low(top)
    middle, low = high_low(rest)
    total_high, total_low = high_low(total)
    for k, column in enumerate((high, middle, low, total_high, total_low)):
        for h in range(heads):
            tile = jnp.where(lane == k * heads + h, column[h * rows : (h + 1) * rows], tile)
    return jnp.concatenate(
        [mixed[h * rows : (h + 1) * rows] for h in range(heads)] + [tile], axis=1
    ).astype(BF16)


def combined(parts_ref, count):
    width = parts_ref.shape[2] - HD
    heads = width // HD
    tops, totals = [], []
    for s in range(count):
        tile = parts_ref[s, :, width:].astype(F32)
        shift = lambda k: pltpu.roll(tile, HD - k * heads, 1)
        tops.append(tile + shift(1) + shift(2))
        totals.append(shift(3) + shift(4))
    top = functools.reduce(jnp.maximum, tops)
    weights = [jnp.exp2((t - top) * EXPONENT) for t in tops]
    total = functools.reduce(jnp.add, [w * t for w, t in zip(weights, totals)])
    outs = []
    for h in range(heads):
        mixed = 0.0
        for s in range(count):
            mixed += weights[s][:, h : h + 1] * parts_ref[s, :, h * HD : (h + 1) * HD].astype(F32)
        outs.append(mixed / total[:, h : h + 1])
    return jnp.concatenate(outs, axis=1)


def kernel(
    kv_count,
    tp_count,
    rows_hbm,
    step_hbm,
    gain_hbm,
    wq_hbm,
    wk_hbm,
    wv_hbm,
    wo_hbm,
    cache_hbm,
    lengths_hbm,
    ids_hbm,
    offsets_hbm,
    rollout_hbm,
    inverse_hbm,
    out_ref,
    step_out_ref,
    rows_ref,
    step_ref,
    gain_ref,
    wq_ref,
    wkv_ref,
    wo_ref,
    cache_ref,
    lengths_ref,
    ids_ref,
    offsets_ref,
    rollout_ref,
    inverse_ref,
    a_send,
    a_recv,
    aux_recv,
    pair_send,
    pair_recv,
    q_recv,
    c_send,
    c_recv,
    cs_recv,
    m_recv,
    e_send,
    e_recv,
    es_recv,
    keys_ref,
    values_ref,
    step_keys_ref,
    step_values_ref,
    local_sem,
    known_sem,
    pair_sem,
    send_sem,
    recv_sem,
):
    me = lax.axis_index("kv")
    tp = lax.axis_index("tp")
    features = rows_ref.shape[1]
    row_count = rows_ref.shape[0]
    width = wq_ref.shape[1]
    heads = width // HD
    share = row_count // kv_count
    block = cache_ref.shape[1]
    total_features = features * kv_count
    partner = tp + 1 - 2 * lax.rem(tp, 2)

    barrier = pltpu.get_barrier_semaphore()
    turn = jnp.where(tp == 0, 1, 0)
    rank = lax.rem(me - turn + kv_count, kv_count)
    of_rank = lambda k: lax.rem(k + turn, kv_count)

    def enter(axis, peer):
        pl.semaphore_signal(barrier, inc=1, device_id={axis: peer}, device_id_type=MESH)

    def greet_above(k, carry):
        enter("kv", of_rank(k))
        return carry

    lax.fori_loop(rank + 1, kv_count, greet_above, 0)

    def greet_tp(j, carry):
        enter("tp", far_first(tp, tp_count, j))
        return carry

    lax.fori_loop(0, tp_count - 1, greet_tp, 0)

    half = wk_hbm.shape[0]
    loads = [
        pltpu.make_async_copy(source, target, local_sem.at[k])
        for k, (source, target) in enumerate(
            (
                (rows_hbm, rows_ref),
                (wq_hbm, wq_ref),
                (wk_hbm, wkv_ref.at[:half]),
                (wv_hbm, wkv_ref.at[half:]),
                (gain_hbm, gain_ref),
                (step_hbm, step_ref),
                (cache_hbm, cache_ref),
                (wo_hbm, wo_ref),
                (lengths_hbm, lengths_ref),
                (ids_hbm, ids_ref),
                (offsets_hbm, offsets_ref),
                (rollout_hbm, rollout_ref),
                (inverse_hbm, inverse_ref),
            )
        )
    ]
    for load in loads:
        load.start()

    pl.semaphore_wait(barrier, rank + tp_count - 1)

    def greet_below(k, carry):
        pl.semaphore_signal(
            known_sem.at[me], inc=1, device_id={"kv": of_rank(k)}, device_id_type=MESH
        )
        return carry

    lax.fori_loop(0, rank, greet_below, 0)

    def remote(phase, axis, peer, source, slot_ref, slot):
        return pltpu.make_async_remote_copy(
            src_ref=source,
            dst_ref=slot_ref.at[slot],
            send_sem=send_sem.at[phase, peer],
            recv_sem=recv_sem.at[phase, slot],
            device_id={axis: peer},
            device_id_type=MESH,
        )

    def to_all(phase, axis, count, here, source, slot_ref):
        def one(j, carry):
            peer = far_first(here, count, j)
            remote(phase, axis, peer, source(peer), slot_ref, here).start()
            return carry

        lax.fori_loop(0, count - 1, one, 0)

    def arrive(phase, axis, peer, slot_ref):
        remote(phase, axis, peer, slot_ref.at[peer], slot_ref, peer).wait_recv()

    def all_arrive(phase, axis, count, here, slot_ref):
        def one(j, carry):
            arrive(phase, axis, far_first(here, count, j), slot_ref)
            return carry

        lax.fori_loop(0, count - 1, one, 0)

    def all_sent(phase, axis, count, here, source, slot_ref):
        def one(j, carry):
            peer = far_first(here, count, j)
            remote(phase, axis, peer, source(peer), slot_ref, here).wait_send()
            return carry

        lax.fori_loop(0, count - 1, one, 0)

    for load in loads[:6]:
        load.wait()
    gain = gain_ref[...].astype(F32).reshape(1, features)
    wide = rows_ref[...].astype(F32)
    normed = (wide * gain).astype(BF16)
    step_wide = jnp.concatenate(
        [step_ref[...].astype(F32), jnp.zeros((HD - SEQS, features), F32)], axis=0
    )
    step_normed = (step_wide[:16] * gain).astype(BF16)
    ones = jnp.ones((8, features), BF16)

    def squares(value):
        high, low = high_low(value * value)
        return dot_t(ones, high.astype(BF16)) + dot_t(ones, low.astype(BF16))

    square_high, square_low = high_low(
        jnp.concatenate([squares(wide), squares(step_wide)], axis=1)
    )
    step_part = jnp.concatenate(
        [dot(step_normed, wq_ref[...])[:8], dot_t(step_normed, wkv_ref[...])[:8]], axis=1
    )
    aux_row = iota(step_part.shape, 0)
    aux = jnp.where(
        aux_row == SEQS, square_high, jnp.where(aux_row == SEQS + 1, square_low, step_part)
    )
    aux_recv[me] = aux[: SEQS + 2].astype(BF16)
    a_send[:, :, :width] = dot(normed, wq_ref[...]).astype(BF16).reshape(kv_count, share, width)
    a_send[:, :, width:] = dot_t(normed, wkv_ref[...]).astype(BF16).reshape(kv_count, share, HD)
    a_recv[me] = a_send[me]

    aux_source = lambda peer: aux_recv.at[me]
    a_source = lambda peer: a_send.at[peer]

    def partials_to(peer):
        remote(0, "kv", peer, aux_source(peer), aux_recv, me).start()
        remote(1, "kv", peer, a_source(peer), a_recv, me).start()

    def send_below(k, carry):
        partials_to(of_rank(k))
        return carry

    def send_above(k, carry):
        peer = of_rank(k)
        pl.semaphore_wait(known_sem.at[peer], 1)
        partials_to(peer)
        return carry

    lax.fori_loop(0, rank, send_below, 0)
    lax.fori_loop(rank + 1, kv_count, send_above, 0)

    for load in loads[6:]:
        load.wait()
    keys_ref[:block, :HD] = cache_ref[SEQS + ids_ref[0], :, :HD]
    keys_ref[:block, HD:] = cache_ref[SEQS + ids_ref[1], :, :HD]
    values_ref[:block, :HD] = cache_ref[SEQS + ids_ref[0], :, HD:]
    values_ref[:block, HD:] = cache_ref[SEQS + ids_ref[1], :, HD:]
    step_keys_ref[:block, :HD] = cache_ref[0, :, :HD]
    step_keys_ref[:block, HD:] = cache_ref[1, :, :HD]
    step_values_ref[:block, :HD] = cache_ref[0, :, HD:]
    step_values_ref[:block, HD:] = cache_ref[1, :, HD:]

    first_count = jnp.sum(
        (rollout_ref[...].reshape(1, row_count) == 0).astype(F32), axis=1, keepdims=True
    )
    offset_0 = offsets_ref[0].astype(F32)
    offset_1 = offsets_ref[1].astype(F32)
    own_row = (iota((share, 1), 0) + me * share).astype(F32)
    position = jnp.where(own_row >= first_count, own_row + offset_1 - first_count, own_row + offset_0)
    step_row = iota((8, 1), 0)
    step_position = jnp.where(step_row == 0, lengths_ref[0], lengths_ref[1]).astype(F32)
    inverse = inverse_ref[...]
    cosine, sine = angles(position, inverse)
    step_cosine, step_sine = angles(step_position, inverse)

    all_arrive(0, "kv", kv_count, me, aux_recv)
    aux_sum = aux_recv[0].astype(F32)
    for s in range(1, kv_count):
        aux_sum += aux_recv[s].astype(F32)
    square_row = aux_sum[SEQS : SEQS + 1] + aux_sum[SEQS + 1 : SEQS + 2]

    def own_scale(start, rows):
        shape = (rows, square_row.shape[1])
        mine = iota(shape, 1) == start + iota(shape, 0)
        squared = jnp.sum(jnp.where(mine, square_row, 0.0), axis=1, keepdims=True)
        return lax.rsqrt(squared / total_features + EPSILON)

    scale = own_scale(me * share, share)
    step_scale = own_scale(row_count, 8)
    step_raw = jnp.concatenate([aux_sum, jnp.zeros_like(aux_sum)], axis=0) * step_scale

    all_arrive(1, "kv", kv_count, me, a_recv)
    raw = a_recv[0].astype(F32)
    for s in range(1, kv_count):
        raw += a_recv[s].astype(F32)
    raw = raw * scale

    pair = jnp.concatenate([raw[:, width:], step_raw[:, width:]], axis=0)
    pair_send[...] = pair
    pair_copy = pltpu.make_async_remote_copy(
        src_ref=pair_send,
        dst_ref=pair_recv,
        send_sem=pair_sem.at[0],
        recv_sem=pair_sem.at[1],
        device_id={"tp": partner},
        device_id_type=MESH,
    )
    pair_copy.start()
    q_recv[me] = jnp.concatenate(
        [rotated(raw[:, at : at + HD], cosine, sine) for at in range(0, width, HD)], axis=1
    ).astype(BF16)
    q_source = lambda peer: q_recv.at[me]
    to_all(2, "kv", kv_count, me, q_source, q_recv)

    step_queries = jnp.concatenate(
        [rotated(step_raw[:, at : at + HD], step_cosine, step_sine) for at in range(0, width, HD)],
        axis=0,
    )

    pair_copy.wait()
    other = pair_recv[...]
    lane = iota(other.shape, 1)
    even = iota(other.shape, 0) * 0 + lax.rem(tp, 2) == 0
    left = jnp.where(even, pair, other)
    right = jnp.where(even, other, pair)
    key_raw = jnp.where(lane < HD // 2, left, pltpu.roll(right, HD // 2, 1))
    value_rows = jnp.where(lane < HD // 2, pltpu.roll(left, HD // 2, 1), right)
    own_keys = rotated(key_raw[:share], cosine, sine)
    step_keys = rotated(key_raw[share:], step_cosine, step_sine)

    def tail(rows):
        filled = jnp.concatenate([rows, jnp.zeros((HD - rows.shape[0], HD), F32)], axis=0)
        return jnp.concatenate([filled, filled], axis=1).astype(BF16)

    keys_ref[block:, :] = tail(own_keys)
    values_ref[block:, :] = tail(value_rows[:share])
    step_keys_ref[block:, :] = tail(step_keys)
    step_values_ref[block:, :] = tail(value_rows[share:])

    key_count = block + HD
    key_lane = iota((1, key_count), 1)
    key_position = key_lane + me * block
    stack_row = iota((heads * 8, 1), 0)
    sequence = lax.rem(stack_row, 8)
    step_limit = jnp.where(sequence == 0, lengths_ref[0], lengths_ref[1])
    own_lane = jnp.where(key_lane * 0 + me == 0, key_lane - block, -1)
    step_allowed = ((key_lane < block) & (key_position < step_limit)) | (own_lane == sequence)
    step_mixed = attend(
        step_queries, sequence > 0, step_allowed, step_keys_ref[...], step_values_ref[...]
    )
    cs_recv[me] = packed(*step_mixed, 8)[:SEQS]
    cs_source = lambda peer: cs_recv.at[me]
    to_all(3, "kv", kv_count, me, cs_source, cs_recv)

    row_in_chunk = lax.rem(iota((heads * share, 1), 0), share)

    def one_chunk(j, carry):
        owner = jnp.where(j == 0, me, far_first(me, kv_count, j - 1))

        @pl.when(j > 0)
        def _():
            arrive(2, "kv", owner, q_recv)

        row = row_in_chunk + owner * share
        second = row.astype(F32) >= first_count
        limit = jnp.where(second, offsets_ref[1], offsets_ref[0])
        tail_key = key_lane[:, block:] - block + me * share
        tail_second = tail_key.astype(F32) >= first_count
        allowed = jnp.concatenate(
            [
                (key_position[:, :block] < limit).astype(F32),
                jnp.where(
                    (tail_key <= row)
                    & (tail_key < (me + 1) * share)
                    & (tail_second.astype(F32) == second.astype(F32)),
                    1.0,
                    0.0,
                ),
            ],
            axis=1,
        )
        queries = stacked(q_recv[owner].astype(F32))
        mixed = attend(queries, second, allowed > 0.5, keys_ref[...], values_ref[...])
        message = packed(*mixed, share)

        @pl.when(j == 0)
        def _():
            c_recv[me] = message

        @pl.when(j > 0)
        def _():
            c_send[owner] = message
            remote(4, "kv", owner, c_send.at[owner], c_recv, me).start()

        return carry

    lax.fori_loop(0, kv_count, one_chunk, 0)

    all_arrive(3, "kv", kv_count, me, cs_recv)
    step_mix = combined(cs_recv, kv_count)
    step_mix = jnp.concatenate([step_mix, jnp.zeros((16 - SEQS, width), F32)], axis=0)
    es_recv[tp] = dot(step_mix.astype(BF16), wo_ref[...])[:SEQS].astype(BF16)
    es_source = lambda peer: es_recv.at[tp]
    to_all(5, "tp", tp_count, tp, es_source, es_recv)

    all_arrive(4, "kv", kv_count, me, c_recv)
    m_recv[me] = combined(c_recv, kv_count).astype(BF16)
    m_source = lambda peer: m_recv.at[me]
    to_all(6, "kv", kv_count, me, m_source, m_recv)

    def one_product(j, carry):
        owner = jnp.where(j == 0, me, far_first(me, kv_count, j - 1))

        @pl.when(j > 0)
        def _():
            arrive(6, "kv", owner, m_recv)

        product = dot(m_recv[owner], wo_ref[...]).astype(BF16)

        @pl.when(owner == tp)
        def _():
            e_recv[tp] = product

        @pl.when(owner != tp)
        def _():
            e_send[owner] = product
            remote(7, "tp", owner, e_send.at[owner], e_recv, tp).start()

        return carry

    lax.fori_loop(0, kv_count, one_product, 0)

    all_arrive(5, "tp", tp_count, tp, es_recv)
    step_total = es_recv[0].astype(F32)
    for s in range(1, tp_count):
        step_total += es_recv[s].astype(F32)
    step_out_ref[...] = step_total.astype(BF16)
    all_arrive(7, "tp", tp_count, tp, e_recv)
    total = e_recv[0].astype(F32)
    for s in range(1, tp_count):
        total += e_recv[s].astype(F32)
    out_ref[...] = total.astype(BF16)

    all_sent(0, "kv", kv_count, me, aux_source, aux_recv)
    all_sent(1, "kv", kv_count, me, a_source, a_recv)
    all_sent(2, "kv", kv_count, me, q_source, q_recv)
    all_sent(3, "kv", kv_count, me, cs_source, cs_recv)
    all_sent(4, "kv", kv_count, me, lambda peer: c_send.at[peer], c_recv)
    all_sent(5, "tp", tp_count, tp, es_source, es_recv)
    all_sent(6, "kv", kv_count, me, m_source, m_recv)
    all_sent(7, "tp", tp_count, tp, lambda peer: e_send.at[peer], e_recv)


def on_device(
    prompt_rows,
    step_rows,
    norm_gain,
    w_query,
    w_key,
    w_value,
    w_output,
    kv_cache,
    step_lengths,
    rollout_ids,
    resume_offsets,
    stretch_rollout,
):
    kv_count = lax.axis_size("kv")
    tp_count = lax.axis_size("tp")
    row_count, features = prompt_rows.shape
    width = w_query.shape[1]
    out_width = w_output.shape[1]
    share = row_count // kv_count
    key_count = kv_cache.shape[1] + HD
    frequency = np.exp(np.arange(HD // 2) * (-2.0 * math.log(THETA) / HD)).astype(np.float32)
    inverse = jnp.asarray(np.concatenate([frequency, frequency])[None, :])
    vmem = pl.BlockSpec(memory_space=pltpu.VMEM)
    anywhere = pl.BlockSpec(memory_space=pl.ANY)
    scratch = [
        pltpu.VMEM(prompt_rows.shape, BF16),
        pltpu.VMEM(step_rows.shape, BF16),
        pltpu.VMEM(norm_gain.shape, BF16),
        pltpu.VMEM(w_query.shape, BF16),
        pltpu.VMEM((HD, features), BF16),
        pltpu.VMEM(w_output.shape, BF16),
        pltpu.VMEM(kv_cache.shape, BF16),
        pltpu.SMEM(step_lengths.shape, jnp.int32),
        pltpu.SMEM(rollout_ids.shape, jnp.int32),
        pltpu.SMEM(resume_offsets.shape, jnp.int32),
        pltpu.VMEM(stretch_rollout.shape, jnp.int32),
        pltpu.VMEM((1, HD), F32),
        pltpu.VMEM((kv_count, share, width + HD), BF16),
        pltpu.VMEM((kv_count, share, width + HD), BF16),
        pltpu.VMEM((kv_count, SEQS + 2, width + HD), BF16),
        pltpu.VMEM((share + 8, HD), F32),
        pltpu.VMEM((share + 8, HD), F32),
        pltpu.VMEM((kv_count, share, width), BF16),
        pltpu.VMEM((kv_count, share, width + HD), BF16),
        pltpu.VMEM((kv_count, share, width + HD), BF16),
        pltpu.VMEM((kv_count, SEQS, width + HD), BF16),
        pltpu.VMEM((kv_count, share, width), BF16),
        pltpu.VMEM((tp_count, share, out_width), BF16),
        pltpu.VMEM((tp_count, share, out_width), BF16),
        pltpu.VMEM((tp_count, SEQS, out_width), BF16),
        pltpu.VMEM((key_count, 2 * HD), BF16),
        pltpu.VMEM((key_count, 2 * HD), BF16),
        pltpu.VMEM((key_count, 2 * HD), BF16),
        pltpu.VMEM((key_count, 2 * HD), BF16),
        pltpu.SemaphoreType.DMA((13,)),
        pltpu.SemaphoreType.REGULAR((kv_count,)),
        pltpu.SemaphoreType.DMA((2,)),
        pltpu.SemaphoreType.DMA((8, kv_count)),
        pltpu.SemaphoreType.DMA((8, kv_count)),
    ]
    return pl.pallas_call(
        functools.partial(kernel, kv_count, tp_count),
        out_shape=(
            jax.ShapeDtypeStruct((share, out_width), BF16),
            jax.ShapeDtypeStruct((step_rows.shape[0], out_width), BF16),
        ),
        in_specs=[anywhere] * 13,
        out_specs=(vmem, vmem),
        scratch_shapes=scratch,
        compiler_params=pltpu.CompilerParams(
            collective_id=0, has_side_effects=True, vmem_limit_bytes=62 * 1024 * 1024
        ),
    )(
        prompt_rows,
        step_rows,
        norm_gain,
        w_query,
        w_key.T,
        w_value.T,
        w_output,
        kv_cache,
        step_lengths,
        rollout_ids,
        resume_offsets,
        stretch_rollout,
        inverse,
    )


def solution(mesh):
    in_specs = (
        P("groups", "kv"),
        P("groups", "kv"),
        P("kv"),
        P("kv", "tp"),
        P("kv", "tp"),
        P("kv", "tp"),
        P("tp", "kv"),
        P("groups", "kv", "tp"),
        P("groups"),
        P("groups"),
        P("groups"),
        P("groups"),
    )
    out_specs = (P(("groups", "tp"), "kv"), P("groups", "kv"))
    return jax.shard_map(
        on_device, mesh=mesh, in_specs=in_specs, out_specs=out_specs, check_vma=False
    )
```
